32 devices in a mesh: kx: 4 (over z), ky: 4 (over x, core), kz: 2 (over y).
Axes of the slice: x: 2, y: 2, z: 4, core: 2. Of those that a mesh axis runs over, the one named last changes fastest.
Arguments:
- offsets: int32 [12, 3], replicated, may hold values from -1 to 1, as said below
- gauge: float32 [2, 4, 4, 4, 256, 256], P(None, 'kx', 'ky', 'kz'), may hold values from -1 to 1, as said below
- intersections: bfloat16 [12, 2, 4, 4, 4, 256, 256], P(None, None, 'kx', 'ky', 'kz'), may hold values from -1 to 1
Outputs:
- new_gauge: float32 [2, 4, 4, 4, 256, 256], P(None, 'kx', 'ky', 'kz')
- centres: float32 [3, 256], replicated
- spread: float32 [], replicated
The draws below stay inside these ranges and needn't reach their ends.
Inputs may be any that keep to these rules, and one draw needn't show every extreme that they name: `offsets`: the 12 rows are the twelve distinct vectors with two entries of magnitude one and one entry zero, each once. `gauge`: every 256 x 256 complex matrix of it is unitary to float32 rounding.
All inputs are finite; a program needn't handle non-finite values.
Results may differ from the reference program's by a relative error of at most 0.0068.
Values may be sent and summed in bfloat16 or wider, within the bound.
A program may use at most 192 MiB of HBM per device.

```python
import math
import jax
import jax.numpy as jnp
import numpy as np
from jax import lax

NW = 256
NB = 12
TERMS = 12
NKX = 4
NKY = 4
NKZ = 4


def draw_offsets(key, part):
    table = np.array([[1, 1, 0], [1, -1, 0], [-1, 1, 0], [-1, -1, 0], [1, 0, 1], [1, 0, -1], [-1, 0, 1], [-1, 0, -1], [0, 1, 1], [0, 1, -1], [0, -1, 1], [0, -1, -1]], dtype=np.int32)
    order = jax.random.permutation(jax.random.fold_in(key, 11), NB)
    return jnp.asarray(table)[order]


def pair_product(left_real, left_imag, right_real, right_imag):
    highest = lax.Precision.HIGHEST
    real = jnp.matmul(left_real, right_real, precision=highest) - jnp.matmul(left_imag, right_imag, precision=highest)
    imag = jnp.matmul(left_real, right_imag, precision=highest) + jnp.matmul(left_imag, right_real, precision=highest)
    return (real, imag)


def draw_gauge(key, part):
    shape = (NKX, NKY, NKZ, NW, NW)
    first_key = jax.random.fold_in(key, 21)
    second_key = jax.random.fold_in(key, 22)
    scale = 0.7 / math.sqrt(NW)
    raw_real = jax.random.normal(first_key, shape, jnp.float32) * scale
    raw_imag = jax.random.normal(second_key, shape, jnp.float32) * scale
    quarter_real = 0.125 * (raw_real - jnp.swapaxes(raw_real, -1, -2))
    quarter_imag = 0.125 * (raw_imag + jnp.swapaxes(raw_imag, -1, -2))
    ident = jnp.broadcast_to(jnp.eye(NW, dtype=jnp.float32), shape)
    term_real, term_imag = (ident, jnp.zeros(shape, jnp.float32))
    total_real, total_imag = (term_real, term_imag)
    for order in range(1, 7):
        term_real, term_imag = pair_product(term_real, term_imag, quarter_real, quarter_imag)
        term_real = term_real / order
        term_imag = term_imag / order
        total_real = total_real + term_real
        total_imag = total_imag + term_imag
    for repeat in range(2):
        total_real, total_imag = pair_product(total_real, total_imag, total_real, total_imag)
    return jnp.stack([total_real, total_imag])


def draw_intersections(key, part):
    shape = (NB, NKX, NKY, NKZ, NW, NW)
    diag_shape = (NB, NKX, NKY, NKZ, NW)
    scale = 0.3 / math.sqrt(NW)
    index_x = jnp.arange(NKX, dtype=jnp.float32)[:, None, None]
    index_y = jnp.arange(NKY, dtype=jnp.float32)[None, :, None]
    index_z = jnp.arange(NKZ, dtype=jnp.float32)[None, None, :]
    flat = index_x * (NKY * NKZ) + index_y * NKZ + index_z
    position = (flat / max(NKX * NKY * NKZ - 1, 1))[None, :, :, :, None]
    off_real = jnp.clip(jax.random.normal(jax.random.fold_in(key, 31), shape, jnp.float32), -4.0, 4.0) * scale
    off_imag = jnp.clip(jax.random.normal(jax.random.fold_in(key, 32), shape, jnp.float32), -4.0, 4.0) * scale
    reach = 0.25 + 0.6 * position
    lowest = 0.7 - 0.4 * position
    fraction = jax.random.uniform(jax.random.fold_in(key, 33), diag_shape, jnp.float32, 0.0, 1.0)
    magnitude = jnp.exp(jnp.log(lowest) * fraction)
    angle = jax.random.uniform(jax.random.fold_in(key, 34), diag_shape, jnp.float32, -1.0, 1.0) * reach
    eye = jnp.eye(NW, dtype=jnp.float32)
    real = off_real * (1.0 - eye) + eye * (magnitude * jnp.cos(angle))[..., None, :]
    imag = off_imag * (1.0 - eye) + eye * (magnitude * jnp.sin(angle))[..., None, :]
    return jnp.stack([real.astype(jnp.bfloat16), imag.astype(jnp.bfloat16)], axis=1)


def setup_inputs(seed: int = 0) -> dict:
    arg_keys = jax.random.split(jax.random.key(seed), 4)
    offsets = draw_offsets(jax.random.fold_in(arg_keys[3], 71), 0)
    gauge = draw_gauge(jax.random.fold_in(arg_keys[3], 71), 0)
    intersections = draw_intersections(jax.random.fold_in(arg_keys[3], 71), 0)
    return dict(offsets=offsets, gauge=gauge, intersections=intersections)


descent_step = 2.0
magnitude_floor = 0.25
highest = lax.Precision.HIGHEST


def transpose_last(matrix):
    return jnp.swapaxes(matrix, -1, -2)


def anti_hermitian(real, imag):
    return 0.5 * (real - transpose_last(real)), 0.5 * (imag + transpose_last(imag))


def skew_part(real, imag):
    return 0.5 * (imag - transpose_last(imag)), -0.5 * (real + transpose_last(real))


def complex_product(left, right):
    real = jnp.matmul(left[0], right[0], precision=highest) - jnp.matmul(left[1], right[1], precision=highest)
    imag = jnp.matmul(left[0], right[1], precision=highest) + jnp.matmul(left[1], right[0], precision=highest)
    return jnp.stack([real, imag])


def exponential(generator):
    size = generator.shape[-1]
    ident = jnp.broadcast_to(jnp.eye(size, dtype=jnp.float32), generator.shape[1:])
    initial = jnp.stack([ident, jnp.zeros_like(ident)])

    def advance(order, carry):
        term, total = carry
        term = complex_product(term, generator) / order.astype(jnp.float32)
        return term, total + term

    final = lax.fori_loop(1, TERMS + 1, advance, (initial, initial))
    return final[1]


def geometry(offsets, counts):
    spacing = jnp.array([2.0 * math.pi / counts[0], 2.0 * math.pi / counts[1], 2.0 * math.pi / counts[2]], jnp.float32)
    bvec = offsets.astype(jnp.float32) * spacing
    weights = 1.0 / (4.0 * jnp.sum(bvec * bvec, axis=1))
    return bvec, weights


def local_terms(m_real, m_imag, bvec, weights):
    diag_real = jnp.diagonal(m_real, axis1=-2, axis2=-1)
    diag_imag = jnp.diagonal(m_imag, axis1=-2, axis2=-1)
    phase = jnp.arctan2(diag_imag, diag_real)
    squared = diag_real * diag_real + diag_imag * diag_imag
    denom = jnp.maximum(squared, magnitude_floor)[..., None, :]
    col_real = diag_real[..., None, :]
    col_imag = diag_imag[..., None, :]
    rot_real = m_real * col_real + m_imag * col_imag
    rot_imag = m_imag * col_real - m_real * col_imag
    hat_real = rot_real / denom
    hat_imag = rot_imag / denom
    sum_rot_real = jnp.einsum("b,b...xy->...xy", weights, rot_real, precision=highest)
    sum_rot_imag = jnp.einsum("b,b...xy->...xy", weights, rot_imag, precision=highest)
    sum_tan_real = jnp.einsum("b,b...y,b...xy->...xy", weights, phase, hat_real, precision=highest)
    sum_tan_imag = jnp.einsum("b,b...y,b...xy->...xy", weights, phase, hat_imag, precision=highest)
    hsum_real = jnp.einsum("b,ba,b...xy->a...xy", weights, bvec, hat_real, precision=highest)
    hsum_imag = jnp.einsum("b,ba,b...xy->a...xy", weights, bvec, hat_imag, precision=highest)
    anti_real, anti_imag = anti_hermitian(sum_rot_real, sum_rot_imag)
    skew_real, skew_imag = skew_part(sum_tan_real, sum_tan_imag)
    return phase, squared, anti_real - skew_real, anti_imag - skew_imag, hsum_real, hsum_imag


def finish(base_real, base_imag, hsum_real, hsum_imag, centres, gauge_block):
    extra_real = jnp.einsum("a...xy,ay->...xy", hsum_real, centres, precision=highest)
    extra_imag = jnp.einsum("a...xy,ay->...xy", hsum_imag, centres, precision=highest)
    skew_real, skew_imag = skew_part(extra_real, extra_imag)
    generator = descent_step * 4.0 * jnp.stack([base_real - skew_real, base_imag - skew_imag])
    return complex_product(gauge_block, exponential(generator))


def reference(offsets, gauge, intersections):
    count_x, count_y, count_z, nbands = gauge.shape[1], gauge.shape[2], gauge.shape[3], gauge.shape[4]
    nvec = offsets.shape[0]
    total_k = count_x * count_y * count_z
    bvec, weights = geometry(offsets, (count_x, count_y, count_z))
    rounded = gauge.astype(jnp.bfloat16)
    zero_index = jnp.zeros((), jnp.int32)

    def point_index(flat):
        return flat // (count_y * count_z), (flat // count_z) % count_y, flat % count_z

    def first_pass(flat):
        index_x, index_y, index_z = point_index(flat)
        own_block = lax.dynamic_slice(rounded, (zero_index, index_x, index_y, index_z, zero_index, zero_index), (2, 1, 1, 1, nbands, nbands)).reshape(2, nbands, nbands).astype(jnp.float32)
        over_block = lax.dynamic_slice(intersections, (zero_index, zero_index, index_x, index_y, index_z, zero_index, zero_index), (nvec, 2, 1, 1, 1, nbands, nbands)).reshape(nvec, 2, nbands, nbands).astype(jnp.float32)
        left_real = jnp.einsum("ia,bie->bae", own_block[0], over_block[:, 0], precision=highest) + jnp.einsum("ia,bie->bae", own_block[1], over_block[:, 1], precision=highest)
        left_imag = jnp.einsum("ia,bie->bae", own_block[0], over_block[:, 1], precision=highest) - jnp.einsum("ia,bie->bae", own_block[1], over_block[:, 0], precision=highest)
        left_real = lax.optimization_barrier(left_real.astype(jnp.bfloat16)).astype(jnp.float32)
        left_imag = lax.optimization_barrier(left_imag.astype(jnp.bfloat16)).astype(jnp.float32)

        def fetch(vector):
            near_x = (index_x + vector[0]) % count_x
            near_y = (index_y + vector[1]) % count_y
            near_z = (index_z + vector[2]) % count_z
            block = lax.dynamic_slice(rounded, (zero_index, near_x, near_y, near_z, zero_index, zero_index), (2, 1, 1, 1, nbands, nbands))
            return block.reshape(2, nbands, nbands)

        neighbour = jax.vmap(fetch)(offsets).astype(jnp.float32)
        m_real = jnp.matmul(left_real, neighbour[:, 0], precision=highest) - jnp.matmul(left_imag, neighbour[:, 1], precision=highest)
        m_imag = jnp.matmul(left_real, neighbour[:, 1], precision=highest) + jnp.matmul(left_imag, neighbour[:, 0], precision=highest)
        return local_terms(m_real, m_imag, bvec, weights)

    points = jnp.arange(total_k, dtype=jnp.int32)
    phase, squared, base_real, base_imag, hsum_real, hsum_imag = lax.map(first_pass, points)
    centres = -jnp.einsum("b,ba,kbn->an", weights, bvec, phase, precision=highest) / total_k
    spread_terms = jnp.einsum("b,kbn->n", weights, 1.0 - squared + phase * phase, precision=highest)
    spread = jnp.sum(spread_terms) / total_k - jnp.sum(centres * centres)

    def second_pass(flat):
        index_x, index_y, index_z = point_index(flat)
        gauge_block = lax.dynamic_slice(gauge, (zero_index, index_x, index_y, index_z, zero_index, zero_index), (2, 1, 1, 1, nbands, nbands)).reshape(2, nbands, nbands)
        return finish(base_real[flat], base_imag[flat], hsum_real[flat], hsum_imag[flat], centres, gauge_block)

    updated = lax.map(second_pass, points)
    new_gauge = updated.reshape(count_x, count_y, count_z, 2, nbands, nbands).transpose(3, 0, 1, 2, 4, 5)
    return new_gauge, centres, spread
```

```python
import functools
import math

import jax
import jax.numpy as jnp
import numpy as np
from jax import lax
from jax.experimental import pallas as pl
from jax.experimental.pallas import tpu as pltpu
from jax.sharding import PartitionSpec as P

TERMS = 12
MAGNITUDE_FLOOR = 0.25
DESCENT_STEP = 2.0
MESH = pl.DeviceIdType.MESH
AXES = ("kx", "ky", "kz")

DIRECTIONS = (
    [(sx, 0, sz) for sx in (-1, 1) for sz in (-1, 1)]
    + [(0, sy, sz) for sy in (-1, 1) for sz in (-1, 1)]
    + [(sx, sy, 0) for sx in (-1, 1) for sy in (-1, 1)]
)


def at(ref, *index):
    return ref.at[index]


def atan2(y, x):
    negative_y = (y < 0) | ((y == 0) & (1.0 / y < 0))
    negative_x = (x < 0) | ((x == 0) & (1.0 / x < 0))
    abs_y, abs_x = jnp.abs(y), jnp.abs(x)
    high, low = jnp.maximum(abs_y, abs_x), jnp.minimum(abs_y, abs_x)
    ratio = jnp.where(high == 0, 0.0, low / jnp.where(high == 0, 1.0, high))
    shifted = ratio > 0.4142135623730950
    t = jnp.where(shifted, (ratio - 1.0) / (ratio + 1.0), ratio)
    z = t * t
    poly = ((8.05374449538e-2 * z - 1.38776856032e-1) * z + 1.99777106478e-1) * z - 3.33329491539e-1
    angle = poly * z * t + t
    angle = jnp.where(shifted, angle + math.pi / 4, angle)
    angle = jnp.where(abs_y > abs_x, math.pi / 2 - angle, angle)
    angle = jnp.where(negative_x, math.pi - angle, angle)
    return jnp.where(negative_y, -angle, angle)


def gather_kernel(
    sizes,
    total_k,
    perm_ref,
    coef_ref,
    own_hbm,
    inter_hbm,
    z_ref,
    centres_ref,
    spread_ref,
    own_ref,
    inter_ref,
    basis_ref,
    left_ref,
    near_ref,
    end_ref,
    m_ref,
    dr_ref,
    di_ref,
    parts_ref,
    sums_x,
    sums_y,
    sums_z,
    local_sem,
    send_sem,
    recv_sem,
    part_send,
    part_recv,
):
    depth = own_ref.shape[0]
    rows = own_ref.shape[1]
    n = rows // 2
    place = [lax.axis_index(axis) for axis in AXES]

    def step(axis, by):
        return {AXES[axis]: lax.rem(place[axis] + by + sizes[axis], sizes[axis])}

    own_copy = pltpu.make_async_copy(own_hbm, own_ref, local_sem.at[0])
    inter_copy = pltpu.make_async_copy(inter_hbm, inter_ref, local_sem.at[1])
    own_copy.start()
    inter_copy.start()

    barrier = pltpu.get_barrier_semaphore()
    partners = 0
    for axis in range(3):
        for by in range(1, sizes[axis]):
            pl.semaphore_signal(barrier, inc=1, device_id=step(axis, by), device_id_type=MESH)
            partners += 1
    pl.semaphore_wait(barrier, partners)

    counter = [0]
    sent = []

    def send(source, target, device):
        index = counter[0]
        counter[0] += 1
        copy = pltpu.make_async_remote_copy(
            src_ref=source,
            dst_ref=target,
            send_sem=send_sem.at[index],
            recv_sem=recv_sem.at[index],
            device_id=device,
            device_id_type=MESH,
        )
        copy.start()
        sent.append(copy)
        return copy

    signs = (-1, 1)
    along_x, along_y, corner, rim = {}, {}, {}, {}
    for j in range(depth):
        for s, sign in enumerate(signs):
            along_x[s, j] = send(own_hbm.at[j], near_ref.at[s, 1 + j], step(0, -sign))
    end = send(own_hbm.at[0], end_ref, step(2, -1))
    for j in reversed(range(depth)):
        for s, sign in enumerate(signs):
            along_y[s, j] = send(own_hbm.at[j], near_ref.at[2 + s, 1 + j], step(1, -sign))

    own_copy.wait()

    def make_basis(j, carry):
        u = own_ref[j].astype(jnp.float32)
        real = u[:n].T
        imag = u[n:].T
        basis_ref[j, :n, :n] = real.astype(jnp.bfloat16)
        basis_ref[j, :n, n:] = imag.astype(jnp.bfloat16)
        basis_ref[j, n:, :n] = (-imag).astype(jnp.bfloat16)
        basis_ref[j, n:, n:] = real.astype(jnp.bfloat16)
        return carry

    lax.fori_loop(0, depth, make_basis, 0)
    inter_copy.wait()

    def make_left(q, carry):
        j = lax.rem(q, depth)
        b = perm_ref[q // depth]
        right = jnp.concatenate([inter_ref[b, 0, j], inter_ref[b, 1, j]], axis=0)
        left = jnp.dot(basis_ref[j], right, preferred_element_type=jnp.float32)
        left_ref[q] = left.astype(jnp.bfloat16)
        return carry

    lax.fori_loop(0, len(DIRECTIONS) * depth, make_left, 0)

    row_id = lax.broadcasted_iota(jnp.int32, (n, n), 0)
    col_id = lax.broadcasted_iota(jnp.int32, (n, n), 1)

    def multiply(direction, j, column, slot):
        q = direction * depth + j
        left = left_ref[q]
        real, imag = left[:n], left[n:]
        full = jnp.concatenate(
            [jnp.concatenate([real, -imag], axis=1), jnp.concatenate([imag, real], axis=1)], axis=0
        )
        m = jnp.dot(full, near_ref[column, slot], preferred_element_type=jnp.float32)
        m_ref[q] = m
        diagonal = row_id == col_id
        dr_ref[pl.ds(q, 1), :] = jnp.sum(jnp.where(diagonal, m[:n], 0.0), axis=0, keepdims=True)
        di_ref[pl.ds(q, 1), :] = jnp.sum(jnp.where(diagonal, m[n:], 0.0), axis=0, keepdims=True)

    def inner_edges(first):
        count = 2 * (depth - 1)

        def body(i, carry):
            s = i // count
            r = lax.rem(i, count)
            up = r // (depth - 1)
            j = lax.rem(r, depth - 1) + 1 - up
            column = first + s
            multiply(2 * column + up, j, column, 1 + j + 2 * up - 1)
            return carry

        if count:
            lax.fori_loop(0, 2 * count, body, 0)

    def outer_edges(first, up):
        j = depth - 1 if up else 0

        def body(s, carry):
            column = first + s
            multiply(2 * column + up, j, column, 1 + j + 2 * up - 1)
            return carry

        lax.fori_loop(0, 2, body, 0)

    for j in reversed(range(depth)):
        for s in range(2):
            along_y[s, j].wait_recv()
            if j == depth - 1:
                rim[1, s, 0] = send(
                    near_ref.at[2 + s, depth], near_ref.at[2 + s, 0], step(2, 1)
                )
    end.wait_recv()
    for s, sign in enumerate(signs):
        rim[1, s, 1] = send(end_ref, near_ref.at[2 + s, depth + 1], step(1, -sign))
    inner_edges(2)

    for j in range(depth):
        for s in range(2):
            along_x[s, j].wait_recv()
            source = near_ref.at[s, 1 + j]
            for other, sign in enumerate(signs):
                corner[s, other, j] = send(
                    source, near_ref.at[4 + 2 * s + other, 1 + j], step(1, -sign)
                )
            if j == depth - 1:
                rim[0, s, 0] = send(source, near_ref.at[s, 0], step(2, 1))
            if j == 0:
                rim[0, s, 1] = send(source, near_ref.at[s, depth + 1], step(2, -1))
    inner_edges(0)

    for up in range(2):
        for s in range(2):
            rim[1, s, up].wait_recv()
        outer_edges(2, up)

    for j in range(depth):
        for s in range(2):
            for other in range(2):
                corner[s, other, j].wait_recv()

        def corners(c, carry, j=j):
            multiply(8 + c, j, 4 + c, 1 + j)
            return carry

        lax.fori_loop(0, 4, corners, 0)

    for up in (1, 0):
        for s in range(2):
            rim[0, s, up].wait_recv()
        outer_edges(0, up)

    dr, di = dr_ref[...], di_ref[...]
    phase = atan2(di, dr)
    squared = dr * dr + di * di
    coef = coef_ref[...]
    weight = coef[:, 0:1]
    weighted = weight * phase
    parts = [
        jnp.sum(coef[:, 1 + a : 2 + a] * weighted, axis=0, keepdims=True) for a in range(3)
    ]
    parts.append(
        jnp.sum(weight * (1.0 - squared + phase * phase), axis=0, keepdims=True)
    )
    parts.append(jnp.zeros((4, n), jnp.float32))
    value = jnp.concatenate(parts, axis=0)
    index = 0
    for axis, slots in enumerate((sums_z, sums_y, sums_x)):
        axis = 2 - axis
        size = sizes[axis]
        me = place[axis]
        parts_ref[axis] = value
        slots[me] = value
        arrivals = []
        for by in range(1, size):
            copy = pltpu.make_async_remote_copy(
                src_ref=parts_ref.at[axis],
                dst_ref=slots.at[me],
                send_sem=part_send.at[index],
                recv_sem=part_recv.at[index],
                device_id=step(axis, by),
                device_id_type=MESH,
            )
            copy.start()
            sent.append(copy)
            source = lax.rem(me + size - by, size)
            arrivals.append(
                pltpu.make_async_remote_copy(
                    src_ref=parts_ref.at[axis],
                    dst_ref=slots.at[source],
                    send_sem=part_send.at[index],
                    recv_sem=part_recv.at[index],
                    device_id=step(axis, by),
                    device_id_type=MESH,
                )
            )
            index += 1
        for copy in arrivals:
            copy.wait_recv()
        value = slots[0]
        for other in range(1, size):
            value = value + slots[other]

    centres = -value[0:3] / total_k
    centres_ref[...] = centres
    per_band = value[3:4] / total_k - jnp.sum(centres * centres, axis=0, keepdims=True)
    spread_ref[...] = jnp.sum(per_band, axis=1, keepdims=True)

    angle = phase
    for a in range(3):
        angle = angle + coef[:, 1 + a : 2 + a] * centres[a : a + 1]
    angle = angle / jnp.maximum(squared, MAGNITUDE_FLOOR)
    dr_ref[...] = weight * (dr + di * angle)
    di_ref[...] = weight * (dr * angle - di)

    strip = 32

    def combine(i, carry):
        j = i // (n // strip)
        start = pl.multiple_of(lax.rem(i, n // strip) * strip, strip)
        real = jnp.zeros((strip, n), jnp.float32)
        imag = jnp.zeros((strip, n), jnp.float32)
        for d in range(len(DIRECTIONS)):
            q = d * depth + j
            cr = dr_ref[pl.ds(q, 1), :]
            ci = di_ref[pl.ds(q, 1), :]
            mr = m_ref[q, pl.ds(start, strip), :]
            mi = m_ref[q, pl.ds(n + start, strip), :]
            real = real + (mr * cr - mi * ci)
            imag = imag + (mr * ci + mi * cr)
        z_ref[j, 0, pl.ds(start, strip), :] = real
        z_ref[j, 1, pl.ds(start, strip), :] = imag
        return carry

    lax.fori_loop(0, depth * (n // strip), combine, 0)

    for copy in sent:
        copy.wait_send()


def split(value):
    high = value.astype(jnp.bfloat16)
    return high, (value - high.astype(jnp.float32)).astype(jnp.bfloat16)


def product(left, right):
    lr, li = split(left[0]), split(left[1])
    rr, ri = split(right[0]), split(right[1])
    n = left[0].shape[0]

    def full(part):
        real, imag = lr[part], li[part]
        return jnp.concatenate(
            [jnp.concatenate([real, -imag], axis=1), jnp.concatenate([imag, real], axis=1)], axis=0
        )

    high, low = full(0), full(1)
    r_high = jnp.concatenate([rr[0], ri[0]], axis=0)
    r_low = jnp.concatenate([rr[1], ri[1]], axis=0)
    out = jnp.dot(high, r_high, preferred_element_type=jnp.float32)
    out = out + (
        jnp.dot(high, r_low, preferred_element_type=jnp.float32)
        + jnp.dot(low, r_high, preferred_element_type=jnp.float32)
    )
    return out[:n], out[n:]


def exponential_kernel(z_ref, gauge_ref, out_ref):
    zr, zi = z_ref[0, 0], z_ref[0, 1]
    n = zr.shape[0]
    scale = 0.5 * DESCENT_STEP * 4.0
    x1 = (scale * (zr - zr.T), scale * (zi + zi.T))
    diagonal = lax.broadcasted_iota(jnp.int32, (n, n), 0) == lax.broadcasted_iota(
        jnp.int32, (n, n), 1
    )
    x2 = product(x1, x1)
    x3 = product(x1, x2)
    x4 = product(x2, x2)
    inverse = [1.0 / math.factorial(k) for k in range(TERMS + 1)]

    def group(first, powers):
        real = jnp.where(diagonal, inverse[first], 0.0)
        imag = jnp.zeros((n, n), jnp.float32)
        for k, power in enumerate(powers):
            real = real + inverse[first + 1 + k] * power[0]
            imag = imag + inverse[first + 1 + k] * power[1]
        return real, imag

    total = group(8, (x1, x2, x3, x4))
    for first in (4, 0):
        scaled = product(x4, total)
        base = group(first, (x1, x2, x3))
        total = (base[0] + scaled[0], base[1] + scaled[1])
    new = product((gauge_ref[0, 0], gauge_ref[1, 0]), total)
    out_ref[0, 0] = new[0]
    out_ref[1, 0] = new[1]


def per_device(sizes, offsets, gauge, intersections):
    depth, n = gauge.shape[3], gauge.shape[4]
    counts = (sizes[0], sizes[1], sizes[2] * depth)
    total_k = counts[0] * counts[1] * counts[2]
    table = np.array(DIRECTIONS, np.float64)
    bvec = table * (2.0 * math.pi / np.array(counts, np.float64))
    weight = 1.0 / (4.0 * np.sum(bvec * bvec, axis=1))
    queue = len(DIRECTIONS) * depth
    coef = np.zeros((queue, 128), np.float32)
    coef[:, 0] = np.repeat(weight, depth)
    coef[:, 1:4] = np.repeat(bvec, depth, axis=0)
    canonical = jnp.array(DIRECTIONS, jnp.int32)
    same = jnp.all(canonical[:, None, :] == offsets[None, :, :], axis=2)
    order = lax.broadcasted_iota(jnp.int32, same.shape, 1)
    perm = jnp.sum(jnp.where(same, order, 0), axis=1)

    flat = gauge.reshape(2, depth, n, n)
    own = jnp.swapaxes(flat.astype(jnp.bfloat16), 0, 1).reshape(depth, 2 * n, n)
    inter = intersections.reshape(len(DIRECTIONS), 2, depth, n, n)
    copies = 5 * depth + 1 + 4 * depth + 8
    bf16, f32 = jnp.bfloat16, jnp.float32
    partners = sum(size - 1 for size in sizes)
    z, centres, spread = pl.pallas_call(
        functools.partial(gather_kernel, sizes, float(total_k)),
        out_shape=(
            jax.ShapeDtypeStruct((depth, 2, n, n), f32),
            jax.ShapeDtypeStruct((3, n), f32),
            jax.ShapeDtypeStruct((1, 1), f32),
        ),
        in_specs=[
            pl.BlockSpec(memory_space=pltpu.SMEM),
            pl.BlockSpec(memory_space=pltpu.VMEM),
            pl.BlockSpec(memory_space=pl.ANY),
            pl.BlockSpec(memory_space=pl.ANY),
        ],
        out_specs=(
            pl.BlockSpec(memory_space=pltpu.VMEM),
            pl.BlockSpec(memory_space=pltpu.VMEM),
            pl.BlockSpec(memory_space=pltpu.VMEM),
        ),
        scratch_shapes=[
            pltpu.VMEM((depth, 2 * n, n), bf16),
            pltpu.VMEM(inter.shape, bf16),
            pltpu.VMEM((depth, 2 * n, 2 * n), bf16),
            pltpu.VMEM((queue, 2 * n, n), bf16),
            pltpu.VMEM((8, depth + 2, 2 * n, n), bf16),
            pltpu.VMEM((2 * n, n), bf16),
            pltpu.VMEM((queue, 2 * n, n), f32),
            pltpu.VMEM((queue, n), f32),
            pltpu.VMEM((queue, n), f32),
            pltpu.VMEM((3, 8, n), f32),
            pltpu.VMEM((sizes[0], 8, n), f32),
            pltpu.VMEM((sizes[1], 8, n), f32),
            pltpu.VMEM((sizes[2], 8, n), f32),
            pltpu.SemaphoreType.DMA((2,)),
            pltpu.SemaphoreType.DMA((copies,)),
            pltpu.SemaphoreType.DMA((copies,)),
            pltpu.SemaphoreType.DMA((partners,)),
            pltpu.SemaphoreType.DMA((partners,)),
        ],
        compiler_params=pltpu.CompilerParams(
            collective_id=0, has_side_effects=True, vmem_limit_bytes=58 * 1024 * 1024
        ),
        name="gather",
    )(perm, jnp.asarray(coef), own, inter)

    updated = pl.pallas_call(
        exponential_kernel,
        grid=(depth,),
        out_shape=jax.ShapeDtypeStruct((2, depth, n, n), f32),
        in_specs=[
            pl.BlockSpec((1, 2, n, n), lambda j: (j, 0, 0, 0)),
            pl.BlockSpec((2, 1, n, n), lambda j: (0, j, 0, 0)),
        ],
        out_specs=pl.BlockSpec((2, 1, n, n), lambda j: (0, j, 0, 0)),
        compiler_params=pltpu.CompilerParams(vmem_limit_bytes=48 * 1024 * 1024),
        name="exponential",
    )(z, flat)
    return updated.reshape(2, 1, 1, depth, n, n), centres, spread.reshape(())


def solution(mesh):
    sizes = tuple(mesh.shape[axis] for axis in AXES)
    return jax.shard_map(
        functools.partial(per_device, sizes),
        mesh=mesh,
        in_specs=(
            P(),
            P(None, "kx", "ky", "kz", None, None),
            P(None, None, "kx", "ky", "kz", None, None),
        ),
        out_specs=(P(None, "kx", "ky", "kz", None, None), P(), P()),
        check_vma=False,
    )
```

```python
import functools
import math

import jax
import jax.numpy as jnp
import numpy as np
from jax import lax
from jax.experimental import pallas as pl
from jax.experimental.pallas import tpu as pltpu
from jax.sharding import PartitionSpec as P

TERMS = 12
MAGNITUDE_FLOOR = 0.25
DESCENT_STEP = 2.0
MESH = pl.DeviceIdType.MESH
AXES = ("kx", "ky", "kz")

DIRECTIONS = (
    [(sx, 0, sz) for sx in (-1, 1) for sz in (-1, 1)]
    + [(0, sy, sz) for sy in (-1, 1) for sz in (-1, 1)]
    + [(sx, sy, 0) for sx in (-1, 1) for sy in (-1, 1)]
)


def atan2(y, x):
    negative_y = (y < 0) | ((y == 0) & (1.0 / y < 0))
    negative_x = (x < 0) | ((x == 0) & (1.0 / x < 0))
    abs_y, abs_x = jnp.abs(y), jnp.abs(x)
    high, low = jnp.maximum(abs_y, abs_x), jnp.minimum(abs_y, abs_x)
    ratio = jnp.where(high == 0, 0.0, low / jnp.where(high == 0, 1.0, high))
    shifted = ratio > 0.4142135623730950
    t = jnp.where(shifted, (ratio - 1.0) / (ratio + 1.0), ratio)
    z = t * t
    poly = ((8.05374449538e-2 * z - 1.38776856032e-1) * z + 1.99777106478e-1) * z - 3.33329491539e-1
    angle = poly * z * t + t
    angle = jnp.where(shifted, angle + math.pi / 4, angle)
    angle = jnp.where(abs_y > abs_x, math.pi / 2 - angle, angle)
    angle = jnp.where(negative_x, math.pi - angle, angle)
    return jnp.where(negative_y, -angle, angle)


def split(value):
    high = value.astype(jnp.bfloat16)
    return high, (value - high.astype(jnp.float32)).astype(jnp.bfloat16)


def prepared(pair):
    return [split(part) for part in (pair[0], pair[1], pair[0] + pair[1])]


def product(left, right):
    real, imag, both = [
        jnp.dot(
            jnp.concatenate([a[0], a[0], a[1]], axis=1),
            jnp.concatenate([b[0], b[1], b[0]], axis=0),
            preferred_element_type=jnp.float32,
        )
        for a, b in zip(left, right)
    ]
    return real - imag, both - real - imag


def exponential_times(gauge, zr, zi):
    n = zr.shape[0]
    scale = 0.5 * DESCENT_STEP * 4.0
    x1 = (scale * (zr - zr.T), scale * (zi + zi.T))
    diagonal = lax.broadcasted_iota(jnp.int32, (n, n), 0) == lax.broadcasted_iota(
        jnp.int32, (n, n), 1
    )
    p1 = prepared(x1)
    x2 = product(p1, p1)
    p2 = prepared(x2)
    x3 = product(p1, p2)
    x4 = product(p2, p2)
    p4 = prepared(x4)
    inverse = [1.0 / math.factorial(k) for k in range(TERMS + 1)]

    def group(first, powers):
        real = jnp.where(diagonal, inverse[first], 0.0)
        imag = 0.0
        for k, power in enumerate(powers):
            real = real + inverse[first + 1 + k] * power[0]
            imag = imag + inverse[first + 1 + k] * power[1]
        return real, imag

    total = group(8, (x1, x2, x3, x4))
    for first in (4, 0):
        scaled = product(p4, prepared(total))
        base = group(first, (x1, x2, x3))
        total = (base[0] + scaled[0], base[1] + scaled[1])
    return product(prepared(gauge), prepared(total))


def step_kernel(
    sizes,
    total_k,
    offsets_ref,
    coef_ref,
    own_hbm,
    inter_hbm,
    gauge_hbm,
    out_ref,
    centres_ref,
    spread_ref,
    perm_ref,
    gauge_ref,
    z_ref,
    own_ref,
    inter_ref,
    basis_ref,
    left_ref,
    near_ref,
    end_ref,
    m_ref,
    dr_ref,
    di_ref,
    parts_ref,
    sums_near,
    sums_far,
    local_sem,
    send_sem,
    recv_sem,
    part_send,
    part_recv,
):
    depth, n = own_ref.shape[1], own_ref.shape[2]
    place = [lax.axis_index(axis) for axis in AXES]

    def moved(axis, by):
        return lax.rem(place[axis] + by + sizes[axis], sizes[axis])

    def step(axis, by):
        return {AXES[axis]: moved(axis, by)}

    plane = [
        (by, bz) for by in range(sizes[1]) for bz in range(sizes[2]) if by or bz
    ]

    own_copy = pltpu.make_async_copy(own_hbm, own_ref, local_sem.at[0])
    inter_copy = pltpu.make_async_copy(inter_hbm, inter_ref, local_sem.at[1])
    own_copy.start()
    inter_copy.start()
    gauge_copy = pltpu.make_async_copy(gauge_hbm, gauge_ref, local_sem.at[2])
    gauge_copy.start()

    barrier = pltpu.get_barrier_semaphore()
    for by, bz in plane:
        pl.semaphore_signal(
            barrier, inc=1, device_id={**step(1, by), **step(2, bz)}, device_id_type=MESH
        )
    for bx in range(1, sizes[0]):
        pl.semaphore_signal(barrier, inc=1, device_id=step(0, bx), device_id_type=MESH)
    pl.semaphore_wait(barrier, len(plane) + sizes[0] - 1)

    counter = [0]
    sent = []

    def send(source, target, device):
        index = counter[0]
        counter[0] += 1
        copy = pltpu.make_async_remote_copy(
            src_ref=source,
            dst_ref=target,
            send_sem=send_sem.at[index],
            recv_sem=recv_sem.at[index],
            device_id=device,
            device_id_type=MESH,
        )
        copy.start()
        sent.append(copy)
        return copy

    signs = (-1, 1)
    along_x, along_y, corner, rim = {}, {}, {}, {}
    for j in range(depth):
        for s, sign in enumerate(signs):
            along_x[s, j] = send(own_hbm.at[:, j], near_ref.at[s, 1 + j], step(0, -sign))
    odd = lax.rem(place[1], 2)
    ends = [
        send(own_hbm.at[:, depth - 1], end_ref.at[0], step(2, 1)),
        send(own_hbm.at[:, 0], end_ref.at[1], step(2, -1)),
    ]
    for j in reversed(range(depth)):
        for s, sign in enumerate(signs):
            along_y[s, j] = send(own_hbm.at[:, j], near_ref.at[2 + s, 1 + j], step(1, -sign))

    own_copy.wait()

    def make_basis(j, carry):
        real = own_ref[0, j].astype(jnp.float32).T
        imag = own_ref[1, j].astype(jnp.float32).T
        basis_ref[j, :n, :n] = real.astype(jnp.bfloat16)
        basis_ref[j, :n, n:] = imag.astype(jnp.bfloat16)
        basis_ref[j, n:, :n] = (-imag).astype(jnp.bfloat16)
        basis_ref[j, n:, n:] = real.astype(jnp.bfloat16)
        return carry

    lax.fori_loop(0, depth, make_basis, 0)
    codes = [
        offsets_ref[b, 0] * 9 + offsets_ref[b, 1] * 3 + offsets_ref[b, 2]
        for b in range(len(DIRECTIONS))
    ]
    for d, (ox, oy, oz) in enumerate(DIRECTIONS):
        found = jnp.int32(0)
        for b, code in enumerate(codes):
            found = found + jnp.where(code == ox * 9 + oy * 3 + oz, b, 0)
        perm_ref[d] = found
    inter_copy.wait()

    def make_left(q, carry):
        j = lax.rem(q, depth)
        b = perm_ref[q // depth]
        right = jnp.concatenate([inter_ref[b, 0, j], inter_ref[b, 1, j]], axis=0)
        left = jnp.dot(basis_ref[j], right, preferred_element_type=jnp.float32)
        left_ref[q] = left.astype(jnp.bfloat16)
        return carry

    lax.fori_loop(0, len(DIRECTIONS) * depth, make_left, 0)

    row_id = lax.broadcasted_iota(jnp.int32, (n, n), 0)
    col_id = lax.broadcasted_iota(jnp.int32, (n, n), 1)

    def multiply(direction, j, column, slot):
        q = direction * depth + j
        left = left_ref[q]
        real, imag = left[:n], left[n:]
        full = jnp.concatenate(
            [jnp.concatenate([real, -imag], axis=1), jnp.concatenate([imag, real], axis=1)], axis=0
        )
        m = jnp.dot(full, near_ref[column, slot].reshape(2 * n, n), preferred_element_type=jnp.float32)
        m_ref[q] = m
        diagonal = row_id == col_id
        dr_ref[pl.ds(q, 1), :] = jnp.sum(jnp.where(diagonal, m[:n], 0.0), axis=0, keepdims=True)
        di_ref[pl.ds(q, 1), :] = jnp.sum(jnp.where(diagonal, m[n:], 0.0), axis=0, keepdims=True)

    def inner_edges(first):
        count = 2 * (depth - 1)

        def body(i, carry):
            s = i // count
            r = lax.rem(i, count)
            up = r // (depth - 1)
            j = lax.rem(r, depth - 1) + 1 - up
            column = first + s
            multiply(2 * column + up, j, column, 1 + j + 2 * up - 1)
            return carry

        if count:
            lax.fori_loop(0, 2 * count, body, 0)

    def outer_edges(first, up):
        j = depth - 1 if up else 0

        def body(s, carry):
            column = first + s
            multiply(2 * column + up, j, column, 1 + j + 2 * up - 1)
            return carry

        lax.fori_loop(0, 2, body, 0)

    for j in reversed(range(depth)):
        for s in range(2):
            along_y[s, j].wait_recv()
        if j:
            for s, sign in enumerate(signs):
                corner[s, 0, j] = send(
                    near_ref.at[2 + odd, 1 + j], near_ref.at[4 + 2 * s + odd, 1 + j], step(0, -sign)
                )
    for up in range(2):
        ends[up].wait_recv()
        for s, sign in enumerate(signs):
            rim[1, s, up] = send(
                end_ref.at[up], near_ref.at[2 + s, (depth + 1) * up], step(1, -sign)
            )
    inner_edges(2)

    for j in range(depth):
        for s in range(2):
            along_x[s, j].wait_recv()
            source = near_ref.at[s, 1 + j]
            if j:
                corner[s, 1, j] = send(
                    source, near_ref.at[4 + 2 * s + odd, 1 + j], step(1, 1 - 2 * odd)
                )
            else:
                for other, sign in enumerate(signs):
                    corner[s, other, j] = send(
                        source, near_ref.at[4 + 2 * s + other, 1 + j], step(1, -sign)
                    )
            if j == depth - 1:
                rim[0, s, 0] = send(source, near_ref.at[s, 0], step(2, 1))
            if j == 0:
                rim[0, s, 1] = send(source, near_ref.at[s, depth + 1], step(2, -1))
    inner_edges(0)

    for up in range(2):
        for s in range(2):
            rim[1, s, up].wait_recv()
        outer_edges(2, up)

    for j in range(depth):
        for s in range(2):
            for other in range(2):
                corner[s, other, j].wait_recv()

        def corners(c, carry, j=j):
            multiply(8 + c, j, 4 + c, 1 + j)
            return carry

        lax.fori_loop(0, 4, corners, 0)

    for up in (1, 0):
        for s in range(2):
            rim[0, s, up].wait_recv()
        outer_edges(0, up)

    dr, di = dr_ref[...], di_ref[...]
    phase = atan2(di, dr)
    squared = dr * dr + di * di
    coef = coef_ref[...]
    weight = coef[:, 0:1]
    weighted = weight * phase
    parts = [
        jnp.sum(coef[:, 1 + a : 2 + a] * weighted, axis=0, keepdims=True) for a in range(3)
    ]
    parts.append(
        jnp.sum(weight * (1.0 - squared + phase * phase), axis=0, keepdims=True)
    )
    parts.append(jnp.zeros((4, n), jnp.float32))
    value = jnp.concatenate(parts, axis=0)
    index = 0
    for stage, slots in enumerate((sums_near, sums_far)):
        if stage == 0:
            me = place[1] * sizes[2] + place[2]
            others = [
                (
                    {**step(1, by), **step(2, bz)},
                    moved(1, -by) * sizes[2] + moved(2, -bz),
                )
                for by, bz in plane
            ]
        else:
            me = place[0]
            others = [(step(0, bx), moved(0, -bx)) for bx in range(1, sizes[0])]
        parts_ref[stage] = value
        slots[me] = value
        arrivals = []
        for device, source in others:
            copies = [
                pltpu.make_async_remote_copy(
                    src_ref=parts_ref.at[stage],
                    dst_ref=slots.at[slot],
                    send_sem=part_send.at[index],
                    recv_sem=part_recv.at[index],
                    device_id=device,
                    device_id_type=MESH,
                )
                for slot in (me, source)
            ]
            copies[0].start()
            sent.append(copies[0])
            arrivals.append(copies[1])
            index += 1
        for copy in arrivals:
            copy.wait_recv()
        value = slots[0]
        for other in range(1, len(others) + 1):
            value = value + slots[other]

    centres = -value[0:3] / total_k
    centres_ref[...] = centres
    per_band = value[3:4] / total_k - jnp.sum(centres * centres, axis=0, keepdims=True)
    spread_ref[...] = jnp.sum(per_band, axis=1, keepdims=True)

    angle = phase
    for a in range(3):
        angle = angle + coef[:, 1 + a : 2 + a] * centres[a : a + 1]
    angle = angle / jnp.maximum(squared, MAGNITUDE_FLOOR)
    dr_ref[...] = weight * (dr + di * angle)
    di_ref[...] = weight * (dr * angle - di)

    strip = 32

    def combine(i, carry):
        j = i // (n // strip)
        start = pl.multiple_of(lax.rem(i, n // strip) * strip, strip)
        real = jnp.zeros((strip, n), jnp.float32)
        imag = jnp.zeros((strip, n), jnp.float32)
        for d in range(len(DIRECTIONS)):
            q = d * depth + j
            cr = dr_ref[pl.ds(q, 1), :]
            ci = di_ref[pl.ds(q, 1), :]
            mr = m_ref[q, pl.ds(start, strip), :]
            mi = m_ref[q, pl.ds(n + start, strip), :]
            real = real + (mr * cr - mi * ci)
            imag = imag + (mr * ci + mi * cr)
        z_ref[j, 0, pl.ds(start, strip), :] = real
        z_ref[j, 1, pl.ds(start, strip), :] = imag
        return carry

    lax.fori_loop(0, depth * (n // strip), combine, 0)

    gauge_copy.wait()

    def update(j, carry):
        new = exponential_times(
            (gauge_ref[0, j], gauge_ref[1, j]), z_ref[j, 0], z_ref[j, 1]
        )
        out_ref[0, j] = new[0]
        out_ref[1, j] = new[1]
        return carry

    lax.fori_loop(0, depth, update, 0)
    for copy in sent:
        copy.wait_send()


def per_device(sizes, offsets, gauge, intersections):
    depth, n = gauge.shape[3], gauge.shape[4]
    counts = (sizes[0], sizes[1], sizes[2] * depth)
    total_k = counts[0] * counts[1] * counts[2]
    table = np.array(DIRECTIONS, np.float64)
    bvec = table * (2.0 * math.pi / np.array(counts, np.float64))
    weight = 1.0 / (4.0 * np.sum(bvec * bvec, axis=1))
    queue = len(DIRECTIONS) * depth
    coef = np.zeros((queue, 128), np.float32)
    coef[:, 0] = np.repeat(weight, depth)
    coef[:, 1:4] = np.repeat(bvec, depth, axis=0)
    flat = gauge.reshape(2, depth, n, n)
    own = flat.astype(jnp.bfloat16)
    inter = intersections.reshape(len(DIRECTIONS), 2, depth, n, n)
    copies = 8 * depth + 10
    bf16, f32 = jnp.bfloat16, jnp.float32
    near = sizes[1] * sizes[2]
    partners = near + sizes[0] - 2
    updated, centres, spread = pl.pallas_call(
        functools.partial(step_kernel, sizes, float(total_k)),
        out_shape=(
            jax.ShapeDtypeStruct((2, depth, n, n), f32),
            jax.ShapeDtypeStruct((3, n), f32),
            jax.ShapeDtypeStruct((1, 1), f32),
        ),
        in_specs=[
            pl.BlockSpec(memory_space=pltpu.SMEM),
            pl.BlockSpec(memory_space=pltpu.VMEM),
            pl.BlockSpec(memory_space=pl.ANY),
            pl.BlockSpec(memory_space=pl.ANY),
            pl.BlockSpec(memory_space=pl.ANY),
        ],
        out_specs=(
            pl.BlockSpec(memory_space=pltpu.VMEM),
            pl.BlockSpec(memory_space=pltpu.VMEM),
            pl.BlockSpec(memory_space=pltpu.VMEM),
        ),
        scratch_shapes=[
            pltpu.SMEM((len(DIRECTIONS),), jnp.int32),
            pltpu.VMEM((2, depth, n, n), f32),
            pltpu.VMEM((depth, 2, n, n), f32),
            pltpu.VMEM((2, depth, n, n), bf16),
            pltpu.VMEM(inter.shape, bf16),
            pltpu.VMEM((depth, 2 * n, 2 * n), bf16),
            pltpu.VMEM((queue, 2 * n, n), bf16),
            pltpu.VMEM((8, depth + 2, 2, n, n), bf16),
            pltpu.VMEM((2, 2, n, n), bf16),
            pltpu.VMEM((queue, 2 * n, n), f32),
            pltpu.VMEM((queue, n), f32),
            pltpu.VMEM((queue, n), f32),
            pltpu.VMEM((2, 8, n), f32),
            pltpu.VMEM((near, 8, n), f32),
            pltpu.VMEM((sizes[0], 8, n), f32),
            pltpu.SemaphoreType.DMA((3,)),
            pltpu.SemaphoreType.DMA((copies,)),
            pltpu.SemaphoreType.DMA((copies,)),
            pltpu.SemaphoreType.DMA((partners,)),
            pltpu.SemaphoreType.DMA((partners,)),
        ],
        compiler_params=pltpu.CompilerParams(
            collective_id=0, has_side_effects=True, vmem_limit_bytes=58 * 1024 * 1024
        ),
        name="step",
    )(offsets, jnp.asarray(coef), own, inter, flat)
    return updated.reshape(2, 1, 1, depth, n, n), centres, spread.reshape(())


def solution(mesh):
    sizes = tuple(mesh.shape[axis] for axis in AXES)
    return jax.shard_map(
        functools.partial(per_device, sizes),
        mesh=mesh,
        in_specs=(
            P(),
            P(None, "kx", "ky", "kz", None, None),
            P(None, None, "kx", "ky", "kz", None, None),
        ),
        out_specs=(P(None, "kx", "ky", "kz", None, None), P(), P()),
        check_vma=False,
    )
```
